256 devices in a mesh: zero: 16 (over z, core), tp: 4 (over y), site: 4 (over x).
Axes of the slice: x: 4, y: 4, z: 8, core: 2. Of those that a mesh axis runs over, the one named last changes fastest.
Arguments:
- weight_gate: float32 [8192, 8192], P(('site', 'zero'), 'tp'), parts along dimension 0, may hold values from -0.1875 to 0.1875
- moment_gate: float32 [8192, 8192], P(('site', 'zero'), 'tp'), parts along dimension 0, may hold values from -0.125 to 0.125
- square_gate: float32 [8192, 8192], P(('site', 'zero'), 'tp'), parts along dimension 0, may hold values from -0.125 to 0.125
- weight_up: float32 [8192, 8192], P(('site', 'zero'), 'tp'), parts along dimension 0, may hold values from -0.1875 to 0.1875
- moment_up: float32 [8192, 8192], P(('site', 'zero'), 'tp'), parts along dimension 0, may hold values from -0.125 to 0.125
- square_up: float32 [8192, 8192], P(('site', 'zero'), 'tp'), parts along dimension 0, may hold values from -0.125 to 0.125
- norm_train: float32 [8192], P(('site', 'zero', 'tp')), parts along dimension 0, may hold values from 0.25 to 1.75
- norm_step: float32 [8192], P(('site', 'zero', 'tp')), parts along dimension 0, may hold values from -0.3 to 0.3
Outputs:
- ready_gate: bfloat16 [8192, 8192], P('site', 'tp'), parts along dimension 0
- ready_up: bfloat16 [8192, 8192], P('site', 'tp'), parts along dimension 0
- scale_gate: float32 [32768], P(('site', 'tp')), parts along dimension 0
- scale_up: float32 [32768], P(('site', 'tp')), parts along dimension 0
- serve_norm: bfloat16 [8192], P('site'), parts along dimension 0
- latest_gate: float32 [8192, 8192], P(('site', 'zero'), 'tp'), parts along dimension 0
- latest_up: float32 [8192, 8192], P(('site', 'zero'), 'tp'), parts along dimension 0
The draws below stay inside these ranges and needn't reach their ends.
There are 4 independent parts, one for each index of `site`. The reference program is written for one: setup_inputs(seed, part) draws one part's arguments, and reference() takes and returns one part's arrays. A program takes and returns all parts, laid end to end along the dimension named above; each array names one. Nothing has to cross between parts.
All inputs are finite; a program needn't handle non-finite values. Where the reference program divides by a largest or mean magnitude, that divisor is 1e-20 or more.
Results may differ from the reference program's by a relative error of at most 0.001.
Values may be sent and summed in bfloat16 or wider, within the bound.
No kernel may reach another device: no remote copies, remote signals or barrier semaphores. Data moves between devices by JAX's collectives and lax.ppermute only.
A program may use at most 128 MiB of HBM per device.

```python
import jax
import jax.numpy as jnp

D_MODEL = 2048
D_INNER = 8192


def with_spikes(values, rng, source, target, shards_of, factor):
    def block_of(dim):
        return (jnp.arange(values.shape[dim]) // (values.shape[dim] // shards_of)).reshape((-1,) + (1,) * (values.ndim - 1 - dim))

    one_side = jax.random.permutation(rng, shards_of)[block_of(target)]
    far = (block_of(target) + shards_of // 2) % shards_of
    return jnp.where((block_of(source) == one_side) | (block_of(source) == far), factor * values, values)


def shard_levels(stream_key, extent, pieces, low, high):
    level = 1.0
    for axis_at, shards_of in pieces:
        steps = jax.random.uniform(jax.random.fold_in(jax.random.fold_in(stream_key, 6), axis_at), (shards_of,), jnp.float32, low / len(pieces), high / len(pieces))
        level = level * jnp.repeat(jnp.exp(steps), extent[axis_at] // shards_of).reshape((-1,) + (1,) * (len(extent) - 1 - axis_at))
    return level


def gaussian(stream_key, shape, spread, reach, shards=(), dtype=jnp.bfloat16):
    values = spread * jax.random.normal(stream_key, shape, jnp.float32)
    if shards:
        values = values * shard_levels(stream_key, shape, shards, -0.22, 0.18)
    return jnp.clip(values, -reach, reach).astype(dtype)


def noise_with(own_key, extent, width, most, cuts, heavy, held_as=jnp.bfloat16):
    values = width * jax.random.normal(own_key, extent, jnp.float32)
    if cuts:
        values = values * shard_levels(own_key, extent, cuts, -0.22, 0.18)
    return jnp.clip(with_spikes(values, jax.random.fold_in(own_key, 3), *heavy), -most, most).astype(held_as)


def setup_inputs(seed: int = 0, part: int = 0) -> dict:
    key_list = jax.random.split(jax.random.key(seed), 9)
    part_splits = jax.random.split(jax.random.fold_in(key_list[8], part), 9)
    return {
        "weight_gate": noise_with(part_splits[0], (D_MODEL, D_INNER), D_MODEL ** -0.5, 0.1875, ((0, 16), (1, 4)), (0, 1, 16, 2.0), jnp.float32),
        "moment_gate": gaussian(part_splits[1], (D_MODEL, D_INNER), D_MODEL ** -0.5, 0.125, ((0, 16), (1, 4)), jnp.float32),
        "square_gate": gaussian(part_splits[2], (D_MODEL, D_INNER), D_MODEL ** -0.5, 0.125, ((0, 16), (1, 4)), jnp.float32),
        "weight_up": noise_with(part_splits[3], (D_MODEL, D_INNER), D_MODEL ** -0.5, 0.1875, ((0, 16), (1, 4)), (0, 1, 16, 2.0), jnp.float32),
        "moment_up": gaussian(part_splits[4], (D_MODEL, D_INNER), D_MODEL ** -0.5, 0.125, ((0, 16), (1, 4)), jnp.float32),
        "square_up": gaussian(part_splits[5], (D_MODEL, D_INNER), D_MODEL ** -0.5, 0.125, ((0, 16), (1, 4)), jnp.float32),
        "norm_train": jnp.clip(1.0 + 0.15 * jax.random.normal(part_splits[6], (D_MODEL,), jnp.float32), 0.25, 1.75),
        "norm_step": jnp.clip(jax.random.uniform(part_splits[7], (D_MODEL,), jnp.float32, -0.3, 0.3) * shard_levels(part_splits[7], (D_MODEL,), ((0, 64),), -0.4, 0.0), -0.3, 0.3),
    }


learn_rate = 0.25
hold_rate = 0.9


def reference(weight_gate, moment_gate, square_gate, weight_up, moment_up, square_up, norm_train, norm_step):
    hold_gate = hold_rate * moment_gate + square_gate
    latest_gate = weight_gate - learn_rate * hold_gate
    hold_up = hold_rate * moment_up + square_up
    latest_up = weight_up - learn_rate * hold_up
    scale_gate = jnp.max(jnp.abs(latest_gate), axis=0)
    ready_gate = (latest_gate / scale_gate).astype(jnp.bfloat16)
    scale_up = jnp.max(jnp.abs(latest_up), axis=0)
    ready_up = (latest_up / scale_up).astype(jnp.bfloat16)
    serve_norm = (norm_train + norm_step).astype(jnp.bfloat16)
    return ready_gate, ready_up, scale_gate, scale_up, serve_norm, latest_gate, latest_up
```

```python
import jax
import jax.numpy as jnp
from jax import lax
from jax.experimental import pallas as pl
from jax.experimental.pallas import tpu as pltpu
from jax.sharding import PartitionSpec as P


learn_rate = 0.25
hold_rate = 0.9

AXIS = "zero"
CORES = 2


def hop(array, step):
    n = lax.axis_size(AXIS) // CORES
    pairs = [(z * CORES + c, (z + step) % n * CORES + c) for z in range(n) for c in range(CORES)]
    return lax.ppermute(array, AXIS, pairs)


def swap(array):
    n = lax.axis_size(AXIS)
    return lax.ppermute(array, AXIS, [(i, i ^ 1) for i in range(n)])


def place(wholes, pieces):
    n = lax.axis_size(AXIS)
    depth = pieces[0][0].shape[0]
    fresh = isinstance(wholes[0], jax.ShapeDtypeStruct)

    def kernel(*refs):
        k = len(pieces)
        ins = refs[:k]
        outs = refs[-3:-1]
        sems = refs[-1]
        me = lax.axis_index(AXIS)
        chip, core = me // CORES, lax.rem(me, CORES)
        copies = []
        for i, (_, which, ahead, over) in enumerate(pieces):
            slot = lax.rem(chip + ahead, n // CORES) * CORES + lax.rem(core + over, CORES)
            rows = pl.ds(pl.multiple_of(slot * depth, depth), depth)
            copies.append(pltpu.make_async_copy(ins[i], outs[which].at[rows, :], sems.at[i]))
        for c in copies:
            c.start()
        for c in copies:
            c.wait()

    k = len(pieces)
    size = sum(p[0].size * 2 for p in pieces)
    anywhere = pl.BlockSpec(memory_space=pl.ANY)
    call = pl.pallas_call(
        kernel,
        out_shape=[jax.ShapeDtypeStruct(w.shape, w.dtype) for w in wholes],
        in_specs=[anywhere] * (k + (0 if fresh else 2)),
        out_specs=[anywhere] * 2,
        scratch_shapes=[pltpu.SemaphoreType.DMA((k,))],
        input_output_aliases={} if fresh else {k: 0, k + 1: 1},
        compiler_params=pltpu.CompilerParams(vmem_limit_bytes=1 << 20),
        cost_estimate=pl.CostEstimate(flops=size, bytes_accessed=2 * size, transcendentals=0),
    )
    args = [p[0] for p in pieces] + ([] if fresh else list(wholes))
    return call(*args)


def settle(wholes, brought):
    pieces = [(a, w, at, 0) for a, w, at in brought]
    pieces += [(swap(a), w, at, 1) for a, w, at in brought]
    return place(wholes, pieces)


def per_device(
    weight_gate, moment_gate, square_gate, weight_up, moment_up, square_up, norm_train, norm_step
):
    hold_gate = hold_rate * moment_gate + square_gate
    latest_gate = weight_gate - learn_rate * hold_gate
    hold_up = hold_rate * moment_up + square_up
    latest_up = weight_up - learn_rate * hold_up
    width = latest_gate.shape[1]
    members = lax.axis_size(AXIS)
    chips = members // CORES
    half = chips // 2

    gain = (norm_train + norm_step).astype(jnp.bfloat16).astype(jnp.float32)
    own = jnp.concatenate(
        [
            jnp.max(jnp.abs(latest_gate), axis=0),
            jnp.max(jnp.abs(latest_up), axis=0),
            jnp.pad(gain, (0, 1024 - gain.shape[0])),
        ]
    )
    notes = {0: own}
    ahead = back = own
    for d in range(1, half + 1):
        back = hop(back, 1)
        notes[chips - d] = back
        if d < half:
            ahead = hop(ahead, -1)
            notes[d] = ahead
    mine = jnp.stack([notes[k] for k in range(chips)])
    theirs = swap(mine)
    top = jnp.max(jnp.maximum(mine, theirs), axis=0)
    scale_gate = top[:width]
    scale_up = top[width : 2 * width]

    narrow_gate = (latest_gate / scale_gate).astype(jnp.bfloat16)
    narrow_up = (latest_up / scale_up).astype(jnp.bfloat16)

    wholes = [jax.ShapeDtypeStruct((members * a.shape[0], width), a.dtype) for a in (narrow_gate, narrow_up)]
    held = {-1: [(narrow_gate, 0, 0), (narrow_up, 1, 0)], 0: [(narrow_up, 1, 0), (narrow_gate, 0, 0)]}
    steps = 2 * half - 1
    for k in range(1, steps + 1):
        d = (k + 1) // 2
        if k >= 3:
            sent = [a for a, _, _ in held[k - 2]]
            sent, wholes = lax.optimization_barrier((sent, list(wholes)))
            held[k - 2] = [(s, w, at) for s, (_, w, at) in zip(sent, held[k - 2])]
        (a, wa, _), (b, wb, _) = held[k - 2]
        held[k] = [(hop(a, 1), wa, chips - d), (hop(b, -1), wb, d)]
        if k != 1 and k != 2:
            wholes = settle(wholes, held[k - 2])
        elif k == 2:
            wholes = settle(wholes, held[-1])
    brought, wholes = lax.optimization_barrier(([a for a, _, _ in held[steps]], list(wholes)))
    held[steps] = [(b, w, at) for b, (_, w, at) in zip(brought, held[steps])]
    for k in (steps - 1, steps):
        wholes = settle(wholes, held[k])

    chip, core = lax.axis_index(AXIS) // CORES, lax.axis_index(AXIS) % CORES
    many = norm_train.shape[0]
    gains = [a[:, 2 * width : 2 * width + many] for a in (mine, theirs)]
    low, high = jnp.where(core == 0, gains[0], gains[1]), jnp.where(core == 0, gains[1], gains[0])
    line = jnp.concatenate([low, high], axis=1)
    line = lax.dynamic_slice_in_dim(jnp.concatenate([line, line]), (chips - chip) % chips, chips, axis=0)
    line = line.reshape(members, many)
    t = lax.axis_size("tp")
    parts = [line]
    for d in range(1, t):
        parts.append(lax.ppermute(line, "tp", [((i + d) % t, i) for i in range(t)]))
    both = jnp.concatenate(parts + parts, axis=1)
    at = (t - lax.axis_index("tp")) % t
    line = lax.dynamic_slice_in_dim(both, at * many, t * many, axis=1)
    serve_norm = line.reshape(-1).astype(jnp.bfloat16)
    return (wholes[0], wholes[1], scale_gate, scale_up, serve_norm, latest_gate, latest_up)


def solution(mesh):
    return shard(mesh, per_device)


def shard(mesh, step):
    placed = (P(("site", "zero"), "tp"),) * 6 + (P(("site", "zero", "tp")),) * 2
    return jax.shard_map(
        step,
        mesh=mesh,
        in_specs=placed,
        out_specs=(
            P("site", "tp"),
            P("site", "tp"),
            P(("site", "tp")),
            P(("site", "tp")),
            P("site"),
            P(("site", "zero"), "tp"),
            P(("site", "zero"), "tp"),
        ),
        check_vma=False,
    )
```

```python
import jax
import jax.numpy as jnp
from jax import lax
from jax.experimental import pallas as pl
from jax.experimental.pallas import tpu as pltpu
from jax.sharding import PartitionSpec as P


learn_rate = 0.25
hold_rate = 0.9

least = 1e-30
lift = 16384.0

AXIS = "zero"
CORES = 2
EXTRA = 8


def between_chips(array, target):
    n = lax.axis_size(AXIS) // CORES
    return lax.ppermute(array, AXIS, [(z * CORES + c, target(z, n) * CORES + c) for z in range(n) for c in range(CORES)])


def hop(array, step):
    return between_chips(array, lambda z, n: (z + step) % n)


def swap(array):
    return lax.ppermute(array, AXIS, [(i, i ^ 1) for i in range(lax.axis_size(AXIS))])


def place(wholes, pieces):
    n = lax.axis_size(AXIS)
    fresh = isinstance(wholes[0], jax.ShapeDtypeStruct)
    depth = wholes[0].shape[0] // n
    arrays = []
    for p in pieces:
        if not any(p[0] is a for a in arrays):
            arrays.append(p[0])
    index = [next(i for i, a in enumerate(arrays) if a is p[0]) for p in pieces]
    k = len(arrays)

    def kernel(*refs):
        ins, outs, sems = refs[:k], refs[-3:-1], refs[-1]
        me = lax.axis_index(AXIS)
        chip, core = me // CORES, lax.rem(me, CORES)

        copies = []
        for i, (_, start, rows, which, ahead, over, at) in enumerate(pieces):
            slot = lax.rem(chip + ahead, n // CORES) * CORES + lax.rem(core + over, CORES)
            there = pl.ds(pl.multiple_of(slot * depth + at, 16), rows)
            here = ins[index[i]].at[pl.ds(start, rows), :]
            copies.append(pltpu.make_async_copy(here, outs[which].at[there, :], sems.at[i]))
        for c in copies:
            c.start()
        for c in copies:
            c.wait()

    size = sum(p[2] * p[0].shape[1] * 2 for p in pieces)
    anywhere = pl.BlockSpec(memory_space=pl.ANY)
    call = pl.pallas_call(
        kernel,
        out_shape=[jax.ShapeDtypeStruct(w.shape, w.dtype) for w in wholes],
        in_specs=[pl.BlockSpec(memory_space=pltpu.VMEM)] * k + [anywhere] * (0 if fresh else 2),
        out_specs=[anywhere] * 2,
        scratch_shapes=[pltpu.SemaphoreType.DMA((len(pieces),))],
        input_output_aliases={} if fresh else {k: 0, k + 1: 1},
        compiler_params=pltpu.CompilerParams(vmem_limit_bytes=8 << 20),
        cost_estimate=pl.CostEstimate(flops=size, bytes_accessed=2 * size, transcendentals=0),
    )
    return list(call(*arrays, *([] if fresh else wholes)))


def tie(arrays, others):
    return lax.optimization_barrier((arrays, others))


def per_device(
    weight_gate, moment_gate, square_gate, weight_up, moment_up, square_up, norm_train, norm_step
):
    hold_gate = hold_rate * moment_gate + square_gate
    latest_gate = weight_gate - learn_rate * hold_gate
    hold_up = hold_rate * moment_up + square_up
    latest_up = weight_up - learn_rate * hold_up
    depth, width = latest_gate.shape
    members = lax.axis_size(AXIS)
    chips = members // CORES
    half = chips // 2

    def coded(latest):
        peak = jnp.max(jnp.abs(latest), axis=0)
        power = jnp.ceil(jnp.log2(jnp.maximum(peak, least)))[None]
        part = latest / jnp.exp2(power)
        return peak, power, part * jnp.abs(part) * lift

    gain = (norm_train + norm_step).astype(jnp.bfloat16)
    many, tps = gain.shape[0], lax.axis_size("tp")
    where = (lax.axis_index(AXIS) * tps + lax.axis_index("tp")) * many
    peak_gate, power_gate, code_gate = coded(latest_gate)
    code_gate = code_gate.astype(jnp.float16)
    (code_gate, power_gate), (peak_gate, latest_gate, where) = tie(
        [code_gate, power_gate], [peak_gate, latest_gate, where]
    )
    spots = lax.broadcasted_iota(jnp.int32, (many, width), 1) - lax.broadcasted_iota(jnp.int32, (many, width), 0) == where
    gains = jnp.dot(gain[None], spots.astype(jnp.bfloat16), preferred_element_type=jnp.float32)[0]
    peak_up, power_up, code_up = coded(latest_up)
    extra = [power_gate, power_up, jnp.zeros((EXTRA - 2, width), jnp.float32)]
    code_up = jnp.concatenate([code_up] + extra).astype(jnp.float16)
    notes = jnp.concatenate([peak_gate, peak_up, gains])
    (code_up, latest_up), (notes,) = tie([code_up, latest_up], [notes])

    def joined(notes, others):
        of_gains = lax.broadcasted_iota(jnp.int32, notes.shape, 0) >= 2 * width
        return jnp.where(of_gains & (notes != 0), notes, jnp.where(of_gains, others, jnp.maximum(notes, others)))

    gate, up = {0: code_gate}, {0: code_up}
    for rows in (gate, up):
        for d in range(1, half):
            rows[chips - d] = hop(rows[(chips - d + 1) % chips], 1)
            rows[d] = hop(rows[d - 1], -1)
        ahead, back = rows[chips - half + 1][: depth // 2], rows[half - 1][depth // 2 :]
        ahead, back = hop(ahead, 1), hop(back, -1)
        rows[half] = jnp.concatenate([ahead, back])

    notes = joined(notes, swap(notes))
    for d in (1, half - 1):
        others = [hop(notes, sign * d) for sign in (1, -1)]
        notes = joined(joined(notes, others[0]), others[1])
    (notes,), _ = tie([notes], [code_up])
    scale_gate, scale_up, gains = notes[:width], notes[width : 2 * width], notes[2 * width :]

    def final(code, power, scale):
        code = code.astype(jnp.float32)
        root = code * lax.rsqrt(jnp.maximum(jnp.abs(code), least))
        ratio = jnp.exp2(power.astype(jnp.float32)) / scale / lift**0.5
        return (root * ratio).astype(jnp.bfloat16)

    wholes = [jax.ShapeDtypeStruct((members * depth, width), jnp.bfloat16)] * 2
    for d in range(half + 1):
        sources = sorted({d, (chips - d) % chips})
        arrays = [a for at in sources for a in (gate[at], up[at])] + [scale_gate, scale_up]
        if d in (0, half):
            (arrays, _) = tie(arrays, [notes])
        else:
            arrays, wholes = tie(arrays, wholes)
        of_gate, of_up = arrays[-2:]
        mine, theirs = [], []
        for i, at in enumerate(sources):
            g, u = arrays[2 * i : 2 * i + 2]
            both = final(g, u[depth], of_gate), final(u[:depth], u[depth + 1], of_up)
            for which, rows in enumerate(both):
                mine.append((rows, 0, depth, which, at, 0, 0))
                theirs.append((swap(rows), 0, depth, which, at, 1, 0))
        if d < half:
            wholes = place(wholes, mine + theirs)
        else:
            wholes = place(place(wholes, mine), theirs)

    line = jnp.broadcast_to(gains[None], (8, width))
    bit = 1
    while bit < tps:
        line = line + lax.ppermute(line, "tp", [(i, i ^ bit) for i in range(tps)])
        bit *= 2
    serve_norm = line[0].astype(jnp.bfloat16)
    return (wholes[0], wholes[1], scale_gate, scale_up, serve_norm, latest_gate, latest_up)


def solution(mesh):
    return shard(mesh, per_device)


def shard(mesh, step):
    placed = (P(("site", "zero"), "tp"),) * 6 + (P(("site", "zero", "tp")),) * 2
    return jax.shard_map(
        step,
        mesh=mesh,
        in_specs=placed,
        out_specs=(
            P("site", "tp"),
            P("site", "tp"),
            P(("site", "tp")),
            P(("site", "tp")),
            P("site"),
            P(("site", "zero"), "tp"),
            P(("site", "zero"), "tp"),
        ),
        check_vma=False,
    )
```
